32 devices in a mesh: groups: 2 (over x), blk: 8 (over z, y), span: 2 (over core).
Axes of the slice: x: 2, y: 2, z: 4, core: 2. Of those that a mesh axis runs over, the one named last changes fastest.
Arguments:
- embeddings: bfloat16 [8192, 768], P(('groups', 'blk', 'span')), parts along dimension 0, may hold values from -6 to 6
- owner_ids: int32 [8192, 1], P(('groups', 'blk', 'span')), parts along dimension 0, may hold values from 0 to 7, as said below
- local_ids: int32 [8192], P(('groups', 'blk', 'span')), parts along dimension 0, may hold values from 0 to 15, as said below
- cluster_map: int32 [256], P('groups'), parts along dimension 0, may hold values from 0 to 127, as said below
Outputs:
- nearest: float32 [8192], P(('groups', 'blk', 'span')), parts along dimension 0
- centroid_cosine: float32 [8192], P(('groups', 'blk', 'span')), parts along dimension 0
The draws below stay inside these ranges and needn't reach their ends.
There are 2 independent parts, one for each index of `groups`. The reference program is written for one: setup_inputs(seed, part) draws one part's arguments, and reference() takes and returns one part's arrays. A program takes and returns all parts, laid end to end along the dimension named above; each array names one. Nothing has to cross between parts.
Inputs may be any that keep to these rules, and one draw needn't show every extreme that they name: `owner_ids`: at most 64 rows of one device name the same owner; in every draw one owner is named by exactly 64 rows of every device. `local_ids`: of the rows of one device that name one owner, at most 16 have local id 0; in every draw one owner receives exactly 16 rows with local id 0 from every device. In every draw some clusters with a local id other than 0 have exactly one row in the whole shard. cluster_map[o * 16 + l] = o * 16 + l for l > 0. For l = 0 the owners fall into runs of 1 to 3 consecutive owners, and every owner of a run has the value of the run's first owner; some run has 3 owners.
All inputs are finite; a program needn't handle non-finite values.
Results may differ from the reference program's by a relative error of at most 0.0017.
Values may be sent and summed in bfloat16 or wider, within the bound.
No kernel may reach another device: no remote copies, remote signals or barrier semaphores. Data moves between devices by JAX's collectives and lax.ppermute only.
A program may use at most 64 MiB of HBM per device.

```python
import jax
import jax.numpy as jnp
from jax import lax

D = 768
ROWS_DEV = 256
OWNED = 16
GIANT_SPAN = 3
ROWS = 4096
CAPACITY = 64
SHARED = 16
CLUSTERS = 128
N_BLK = 8
N_SPAN = 2


def routing(key):
    keys = jax.random.split(key, 9)
    devices = N_BLK * N_SPAN
    candidates = N_BLK * CAPACITY
    owner_range = jnp.arange(N_BLK, dtype=jnp.int32)
    busy = jax.random.randint(keys[0], (), 0, N_BLK)
    slot_owner = jnp.arange(candidates, dtype=jnp.int32) // CAPACITY
    slot_rank = jnp.arange(candidates, dtype=jnp.int32) % CAPACITY
    weights = jax.random.randint(keys[1], (devices, N_BLK), 0, 8192)
    weights = jnp.where(owner_range[None, :] == busy, 1 << 20, weights)
    noise = jax.random.randint(keys[2], (devices, candidates), 0, 4096)
    score = (noise + weights[:, slot_owner]) * candidates + jnp.arange(candidates, dtype=jnp.int32)[None, :]
    chosen = jnp.argsort(-score, axis=1)[:, :ROWS_DEV]
    shuffle = jax.vmap(lambda k: jax.random.permutation(k, ROWS_DEV))(jax.random.split(keys[3], devices))
    chosen = jnp.take_along_axis(chosen, shuffle, axis=1)
    owners = slot_owner[chosen]
    ranks = slot_rank[chosen]
    share_count = jax.random.randint(keys[4], (devices, N_BLK), 0, SHARED + 1)
    share_count = jnp.where(owner_range[None, :] == busy, SHARED, share_count)
    shared = ranks < jnp.take_along_axis(share_count, owners, axis=1)
    lone = jax.random.randint(keys[5], (N_BLK,), 1, OWNED)
    flagged = (jax.random.randint(keys[6], (N_BLK,), 0, 2) == 1) | (owner_range == busy)
    first_pick = jax.random.randint(keys[7], (devices, ROWS_DEV), 0, OWNED - 2)
    second_pick = jax.random.randint(keys[8], (devices, ROWS_DEV), 0, OWNED - 2)
    skewed = jnp.minimum(first_pick, second_pick).reshape(ROWS)
    owner_flat = owners.reshape(ROWS).astype(jnp.int32)
    shared_flat = shared.reshape(ROWS)
    lone_row = lone[owner_flat]
    other = 1 + (lone_row + skewed) % (OWNED - 1)
    row_index = jnp.arange(ROWS, dtype=jnp.int32)
    open_rows = (owner_flat[:, None] == owner_range[None, :]) & jnp.logical_not(shared_flat)[:, None]
    first_row = jnp.min(jnp.where(open_rows, row_index[:, None], ROWS), axis=0)
    single = flagged[owner_flat] & (first_row[owner_flat] == row_index)
    local = jnp.where(shared_flat, 0, jnp.where(single, lone_row, other))
    return (owner_flat.reshape(ROWS, 1).astype(jnp.int32), local.astype(jnp.int32))


def draw_owner_ids(key, part):
    return routing(jax.random.fold_in(key, 11))[0]


def draw_local_ids(key, part):
    return routing(jax.random.fold_in(key, 11))[1]


def draw_cluster_map(key, part):
    first, second = jax.random.split(jax.random.fold_in(key, 7))
    lengths = jax.random.randint(first, (N_BLK,), 1, GIANT_SPAN + 1)
    forced = jax.random.randint(second, (), 0, max(1, N_BLK // GIANT_SPAN - 1))
    owner = jnp.arange(N_BLK, dtype=jnp.int32)
    lengths = jnp.where(owner == forced, GIANT_SPAN, lengths)
    starts = jnp.cumsum(lengths) - lengths
    inside = starts[None, :] <= owner[:, None]
    run_start = jnp.max(jnp.where(inside, starts[None, :], 0), axis=1)
    local = jnp.arange(OWNED, dtype=jnp.int32)
    base = owner[:, None] * OWNED + local[None, :]
    merged = jnp.where(local[None, :] == 0, run_start[:, None] * OWNED, base)
    return merged.reshape(CLUSTERS).astype(jnp.int32)


def level_of(stream_key, shape, pieces, low, high):
    def one(position, blocks):
        draws = jax.random.uniform(jax.random.fold_in(jax.random.fold_in(stream_key, 6), position), (blocks,), jnp.float32, low / len(pieces), high / len(pieces))
        return jnp.repeat(jnp.exp(draws), shape[position] // blocks).reshape((-1,) + (1,) * (len(shape) - position - 1))

    loudness = one(*pieces[0])
    for cut in pieces[1:]:
        loudness = loudness * one(*cut)
    return loudness


def gaussian(key, dims, deviation, bound, shards=(), kind=jnp.bfloat16):
    result = jax.random.normal(key, dims, jnp.float32) * deviation
    if len(shards) > 0:
        result = level_of(key, dims, shards, -0.22, 0.18) * result
    return jnp.clip(result, min=-bound, max=bound).astype(kind)


def setup_inputs(seed: int = 0, part: int = 0) -> dict:
    key_list = jax.random.split(jax.random.key(seed), 5)
    part_splits = jax.random.split(jax.random.fold_in(key_list[4], part), 5)
    embeddings = gaussian(part_splits[0], (ROWS, D), 1.0, 6.0, ((0, 16),))
    owner_ids = draw_owner_ids(jax.random.fold_in(jax.random.fold_in(key_list[4], part), 71), part)
    local_ids = draw_local_ids(jax.random.fold_in(jax.random.fold_in(key_list[4], part), 71), part)
    cluster_map = draw_cluster_map(jax.random.fold_in(jax.random.fold_in(key_list[4], part), 71), part)
    return {"embeddings": embeddings, "owner_ids": owner_ids, "local_ids": local_ids, "cluster_map": cluster_map}


def normalize(values):
    wide = values.astype(jnp.float32)
    scale = lax.rsqrt(lax.optimization_barrier(jnp.sum(wide * wide, axis=1, keepdims=True)) + 1e-06)
    return (wide * scale).astype(jnp.bfloat16)

def reference(embeddings, owner_ids, local_ids, cluster_map):
    unit = normalize(embeddings)
    flat = (owner_ids[:, 0] * OWNED + local_ids).astype(jnp.int32)
    cluster = cluster_map[flat].astype(jnp.int32)
    wide = unit.astype(jnp.float32)
    sums = jax.ops.segment_sum(wide, cluster, num_segments=CLUSTERS)
    length = jnp.sqrt(lax.optimization_barrier(jnp.sum(sums * sums, axis=1, keepdims=True)))
    direction = sums / jnp.maximum(length, 1.0)
    centroid_cosine = lax.optimization_barrier(jnp.sum(wide * direction[cluster], axis=1))
    total = unit.shape[0]
    every = jnp.arange(total, dtype=jnp.int32)

    def one_block(start):
        piece = lax.dynamic_slice_in_dim(unit, start, ROWS_DEV, 0)
        tags = lax.dynamic_slice_in_dim(cluster, start, ROWS_DEV, 0)
        scores = jnp.dot(piece, unit.T, preferred_element_type=jnp.float32)
        index = start + jnp.arange(ROWS_DEV, dtype=jnp.int32)
        keep = (tags[:, None] == cluster[None, :]) & (index[:, None] != every[None, :])
        return lax.optimization_barrier(jnp.max(jnp.where(keep, scores, -1.0), axis=1))
    starts = jnp.arange(total // ROWS_DEV, dtype=jnp.int32) * ROWS_DEV
    nearest = lax.map(one_block, starts).reshape(total)
    return (nearest, centroid_cosine)
```

```python
import jax
import jax.numpy as jnp
from jax import lax
from jax.experimental import pallas as pl
from jax.experimental.pallas import tpu as pltpu
from jax.sharding import PartitionSpec as P

F32 = jnp.float32
BF16 = jnp.bfloat16
I32 = jnp.int32
NT = (((1,), (1,)), ((), ()))


class Sizes:
    def __init__(self, owners, rows, width, clusters):
        self.owners, self.rows, self.width = owners, rows, width
        self.owned = clusters // owners
        self.own = 2 * rows // owners
        self.help = -(-(self.own // 4) // 8) * 8
        self.block = self.own + self.help + 8
        self.n_own = owners * self.own
        self.n_help = owners * self.help
        self.lanes = self.n_own + self.n_help
        assert owners & (owners - 1) == 0 and self.lanes <= width


def iota(shape, axis):
    return lax.broadcasted_iota(I32, shape, axis)


def dot(left, right):
    return jnp.dot(left, right, preferred_element_type=F32)


def dot_nt(left, right):
    return lax.dot_general(left, right, NT, preferred_element_type=F32)


def shared_heads(z, map_ref):
    return [map_ref[o * z.owned] for o in range(z.owners)]


def column(z, values):
    index = iota((z.owners, 1), 0)
    out = jnp.zeros((z.owners, 1), I32)
    for o, value in enumerate(values):
        out = jnp.where(index == o, value, out)
    return out


def pack_kernel(z, map_ref, x_ref, owner_ref, local_ref, info_ref, *out_refs):
    me = lax.axis_index("blk")
    wide = x_ref[...].astype(F32)
    scale = lax.rsqrt(jnp.sum(wide * wide, axis=1, keepdims=True) + 1e-06)
    unit = (wide * scale).astype(BF16)
    owner = owner_ref[...]
    local = local_ref[...]
    shape = (z.owners, z.rows)
    named = iota(shape, 0) == owner
    shared = named & (local == 0)
    heads = shared_heads(z, map_ref)
    helpers = []
    for o in range(z.owners):
        helper = jnp.int32(0)
        if o >= 2:
            helper = jnp.where(heads[o - 2] == heads[o], o - 2 + 1, helper)
        if o + 1 < z.owners:
            helper = jnp.where(heads[o + 1] == heads[o], o + 1 + 1, helper)
        helpers.append(helper)
    helper = jnp.sum(jnp.where(shared, column(z, helpers), 0), axis=0, keepdims=True)
    earlier = (iota((z.rows, z.rows), 0) < iota((z.rows, z.rows), 1)).astype(F32).astype(BF16)
    both = jnp.concatenate([named.astype(F32), shared.astype(F32)], axis=0).astype(BF16)
    before = dot(both, earlier)
    rank = jnp.sum(jnp.where(named, before[: z.owners], 0.0), axis=0, keepdims=True).astype(I32)
    rank0 = jnp.sum(jnp.where(shared, before[z.owners :], 0.0), axis=0, keepdims=True).astype(I32)
    rel = owner ^ me
    hrel = jnp.where(helper > 0, (helper - 1) ^ me, -1)
    pos = rel * z.block + rank
    hpos = jnp.where(helper > 0, hrel * z.block + z.own + rank0, -1)
    slot = iota((z.owners * z.block, z.rows), 0)
    pick = jnp.where((slot == pos) | (slot == hpos), 1.0, 0.0).astype(BF16)
    packed = dot(pick, unit).astype(BF16)
    tpos = rel * z.own + rank
    thpos = jnp.where(helper > 0, z.n_own + hrel * z.help + rank0, -1)
    lane = iota((z.lanes, z.rows), 0)
    pick_tag = jnp.where((lane == tpos) | (lane == thpos), 1.0, 0.0).astype(BF16)
    weight = jnp.where(iota(shape, 0) == rel, local + 1, 0).astype(F32).astype(BF16)
    helped = jnp.where(iota(shape, 0) == hrel, 1.0, 0.0).astype(BF16)
    tags = jnp.concatenate(
        [dot_nt(weight, pick_tag[: z.n_own]), dot_nt(helped, pick_tag[z.n_own :])], axis=1
    )
    filled = jnp.zeros((8, z.width - z.lanes), BF16) if z.width > z.lanes else None
    for s in range(z.owners):
        out = out_refs[s]
        out[: z.block - 8, :] = packed[s * z.block : (s + 1) * z.block - 8]
        out[z.block - 8 :, : z.lanes] = jnp.broadcast_to(tags[s : s + 1], (8, z.lanes)).astype(BF16)
        if filled is not None:
            out[z.block - 8 :, z.lanes :] = filled
    info = jnp.concatenate([pos * 0 + tpos, helper, thpos, local], axis=0)
    info_ref[...] = jnp.concatenate([info, info], axis=0)


def score_kernel(z, *refs):
    mine, other = refs[: z.owners], refs[z.owners : 2 * z.owners]
    ret_ref, own_ref, help_ref = refs[2 * z.owners :]
    me = lax.axis_index("blk")
    tags = []
    for half, blocks in enumerate((mine, other)):
        total = jnp.zeros((8, z.lanes), F32)
        for s, block in enumerate(blocks):
            own_ref[pl.ds(half * z.n_own + s * z.own, z.own), :] = block[: z.own, :]
            help_ref[pl.ds(half * z.n_help + s * z.help, z.help), :] = block[z.own : z.own + z.help, :]
            total += block[z.own + z.help :, : z.lanes].astype(F32)
        tags.append(total[:1])
    own_row = jnp.concatenate([t[:, : z.n_own] for t in tags], axis=1)
    help_row = jnp.concatenate([t[:, z.n_own :] for t in tags], axis=1)

    def columns(row):
        pieces = [row[:, i : i + 128] for i in range(0, row.shape[1], 128)]
        while len(pieces) < 8:
            pieces.append(jnp.zeros((1, 128), F32))
        return jnp.concatenate(pieces, axis=0).T

    own_cols, help_cols = columns(own_row), columns(help_row)
    my_own = jnp.where(own_row[:, : z.n_own] > 0, own_row[:, : z.n_own], -1.0)
    my_help = jnp.where(help_row[:, : z.n_help] > 0, help_row[:, : z.n_help], -1.0)
    rows_own = own_ref[: z.n_own, :]
    rows_help = help_ref[: z.n_help, :]

    def masked(keys, cols, first, rows, row_tags, skip_self):
        scores = dot_nt(keys, rows)
        best = None
        for q in range(keys.shape[0] // 128):
            piece = scores[q * 128 : (q + 1) * 128]
            keep = cols[:, first + q : first + q + 1] == row_tags
            if skip_self:
                keep &= iota(piece.shape, 0) + q * 128 != iota(piece.shape, 1)
            piece = jnp.where(keep, piece, -1.0)
            piece = jnp.max(piece.reshape(16, 8, piece.shape[1]), axis=0)
            best = piece if best is None else jnp.maximum(best, piece)
        return best

    half = z.n_own // 128
    keys0, keys1 = own_ref[: z.n_own, :], own_ref[z.n_own :, :]
    best_own = jnp.maximum(
        masked(keys0, own_cols, 0, rows_own, my_own, True),
        masked(keys1, own_cols, half, rows_own, my_own, False),
    )
    best_own = jnp.maximum(best_own, masked(help_ref[...], help_cols, 0, rows_own, my_own, False))
    best_help = jnp.maximum(
        masked(keys0, own_cols, 0, rows_help, my_help, False),
        masked(keys1, own_cols, half, rows_help, my_help, False),
    )
    best_own = jnp.max(best_own, axis=0, keepdims=True)
    best_help = jnp.max(best_help, axis=0, keepdims=True)

    owned = z.owned
    chosen = (iota((owned, 2 * z.n_own), 0) + 1).astype(F32) == own_row
    sums = dot(jnp.where(chosen, 1.0, 0.0).astype(BF16), own_ref[...])
    helped = (iota((owned, 2 * z.n_help), 0) + 1).astype(F32) == help_row
    extra = dot(jnp.where(helped, 1.0, 0.0).astype(BF16), help_ref[...])
    square = jnp.sum(sums * (sums + 2.0 * extra), axis=1, keepdims=True)
    inverse = 1.0 / jnp.maximum(jnp.sqrt(jnp.maximum(square, 0.0)), 1.0)
    inverse = jnp.where(iota((owned, 1), 0) == 0, 1.0, inverse)
    both = jnp.concatenate([sums + extra, sums], axis=0)
    high = both.astype(BF16)
    low = (both - high.astype(F32)).astype(BF16)
    parts = jnp.concatenate([high, low], axis=0)
    along = dot_nt(parts, rows_own)
    along = (along[:owned] + along[2 * owned : 3 * owned]) * inverse
    hits = (iota((owned, z.n_own), 0) + 1).astype(F32) == my_own
    value_own = jnp.sum(jnp.where(hits, along, 0.0), axis=0, keepdims=True)
    along = dot_nt(parts, rows_help)
    value_help = along[owned : owned + 1] + along[3 * owned : 3 * owned + 1]
    shared_square = jnp.broadcast_to(square[:1], (1, 128))
    for s in range(z.owners):
        o = s * z.own // 128 * 128
        h = s * z.help // 128 * 128
        parts = [
            best_own[:, o : o + 128],
            best_help[:, h : h + 128],
            value_own[:, o : o + 128],
            value_help[:, h : h + 128],
        ] + [shared_square] * 4
        ret_ref[me ^ s] = jnp.concatenate(parts, axis=0)


def finish_kernel(z, map_ref, ret_ref, info_ref, owner_ref, nearest_ref, cosine_ref):
    owner = owner_ref[...]
    tpos, helper, thpos, local = (info_ref[i : i + 1, :] for i in range(4))
    back = ret_ref[...].reshape(z.owners * 8, 128).T
    slot = iota((128, z.rows), 0)
    own_slot = jnp.where(slot == tpos % 128, owner, -1)
    help_slot = jnp.where(slot == thpos % 128, helper - 1, -1)
    best = jnp.full((128, z.rows), -1.0, F32)
    value = jnp.zeros((128, z.rows), F32)
    for d in range(z.owners):
        mine = own_slot == d
        extra = help_slot == d
        best = jnp.maximum(best, jnp.where(mine, back[:, 8 * d : 8 * d + 1], -1.0))
        best = jnp.maximum(best, jnp.where(extra, back[:, 8 * d + 1 : 8 * d + 2], -1.0))
        value += jnp.where(mine, back[:, 8 * d + 2 : 8 * d + 3], 0.0)
        value += jnp.where(extra, back[:, 8 * d + 3 : 8 * d + 4], 0.0)
    best = jnp.max(best, axis=0, keepdims=True)
    value = jnp.sum(value, axis=0, keepdims=True)
    heads = column(z, shared_heads(z, map_ref))
    named = iota((z.owners, z.rows), 0) == owner
    head = jnp.sum(jnp.where(named, heads, 0), axis=0, keepdims=True)
    squares = ret_ref[:, 4, :][:, :1]
    square = jnp.sum(jnp.where(heads == head, squares, 0.0), axis=0, keepdims=True)
    shared = value / jnp.maximum(jnp.sqrt(jnp.maximum(square, 0.0)), 1.0)
    nearest_ref[...] = best
    cosine_ref[...] = jnp.where(local == 0, shared, value)


def body(embeddings, owner_ids, local_ids, cluster_map):
    rows, width = embeddings.shape
    n = lax.axis_size("blk")
    z = Sizes(n, rows, width, cluster_map.shape[0])
    vmem = pl.BlockSpec(memory_space=pltpu.VMEM)
    smem = pl.BlockSpec(memory_space=pltpu.SMEM)
    owner = owner_ids.reshape(1, rows)
    local = local_ids.reshape(1, rows)
    block = jax.ShapeDtypeStruct((z.block, width), BF16)
    limit = pltpu.CompilerParams(vmem_limit_bytes=24 * 2**20)
    packed = pl.pallas_call(
        lambda *refs: pack_kernel(z, *refs),
        out_shape=[jax.ShapeDtypeStruct((8, rows), I32)] + [block] * n,
        in_specs=[smem, vmem, vmem, vmem],
        out_specs=[vmem] * (n + 1),
        compiler_params=limit,
        name="pack",
    )(cluster_map, embeddings, owner, local)
    info, blocks = packed[0], packed[1:]
    swap = [(0, 1), (1, 0)]
    order = sorted(range(1, n), key=lambda s: -(s.bit_length()))
    mine = {0: blocks[0]}
    for s in order:
        mine[s] = lax.ppermute(blocks[s], "blk", [(i, i ^ s) for i in range(n)])
    other = {s: lax.ppermute(mine[s], "span", swap) for s in range(n)}
    ret = pl.pallas_call(
        lambda *refs: score_kernel(z, *refs),
        out_shape=jax.ShapeDtypeStruct((n, 8, 128), F32),
        in_specs=[vmem] * (2 * n),
        out_specs=vmem,
        scratch_shapes=[
            pltpu.VMEM((2 * z.n_own, width), BF16),
            pltpu.VMEM((2 * z.n_help, width), BF16),
        ],
        compiler_params=limit,
        name="score",
    )(*[mine[s] for s in range(n)], *[other[s] for s in range(n)])
    back = lax.all_to_all(ret, "blk", split_axis=0, concat_axis=0, tiled=True)
    row = jax.ShapeDtypeStruct((1, rows), F32)
    nearest, cosine = pl.pallas_call(
        lambda *refs: finish_kernel(z, *refs),
        out_shape=[row, row],
        in_specs=[smem, vmem, vmem, vmem],
        out_specs=[vmem, vmem],
        compiler_params=limit,
        name="finish",
    )(cluster_map, back, info, owner)
    return nearest.reshape(rows), cosine.reshape(rows)


def solution(mesh):
    return jax.shard_map(
        body,
        mesh=mesh,
        in_specs=(
            P(("groups", "blk", "span"), None),
            P(("groups", "blk", "span"), None),
            P(("groups", "blk", "span")),
            P("groups"),
        ),
        out_specs=(P(("groups", "blk", "span")), P(("groups", "blk", "span"))),
        check_vma=False,
    )
```
